32 devices in a mesh: rel: 4 (over y, x), tgt: 8 (over z, core).
Axes of the slice: x: 2, y: 2, z: 4, core: 2. Of those that a mesh axis runs over, the one named last changes fastest.
Arguments:
- features: bfloat16 [2048, 768], P('tgt'), may hold values from -6 to 6
- weights: bfloat16 [8, 768, 768], P('rel'), may hold values from -0.109375 to 0.109375
- bias: float32 [768], replicated, may hold values from -3 to 3
- cotangent: bfloat16 [2048, 768], P('tgt'), may hold values from -1.0546875 to 1.0546875
- tile_values: int32 [8, 2048, 8, 128], P('rel', 'tgt'), may hold values from 0 to 3, as said below
- tile_count: int32 [8, 16], P('rel', 'tgt'), may hold values from 1 to 8, as said below
- tile_slot: int32 [8, 16, 8], P('rel', 'tgt'), may hold values from 0 to 7, as said below
- source_blocks: int32 [8, 8], replicated, may hold values from -1 to 1, as said below
Outputs:
- output: bfloat16 [2048, 768], P('tgt', 'rel')
- grad_weights: float32 [8, 768, 768], P('rel', 'tgt')
- grad_features: float32 [16, 128, 768], P('tgt', 'rel')
The draws below stay inside these ranges and needn't reach their ends.
Inputs may be any that keep to these rules, and one draw needn't show every extreme that they name: `tile_values`: entries in tile slots at or beyond the live count are arbitrary and take no part. `tile_count`: every relation has some tile row of targets with all 8 slots live. `tile_slot`: every tile slot, live or not, names an owner for which the target block's entry of source_blocks is not -1. `source_blocks`: entry [t, o] is a block index within owner o's 2 blocks, or -1 where target block t reads nothing from o; entry [t, t] is never -1.
All inputs are finite; a program needn't handle non-finite values.
Results may differ from the reference program's by a relative error of at most 0.01.
Values may be sent and summed in bfloat16 or wider, within the bound.
A program may use at most 64 MiB of HBM per device.

```python
import jax
import jax.numpy as jnp
from jax import lax

D = 768
BLK = 128
SLOTS = 8
REL_DEV = 2
TGT_DEV = 256
REL = 8
OWNERS = 8
NODES = 2048
N_REL = 4


def source_table(key):
    picked = jax.random.randint(jax.random.fold_in(key, 11), (OWNERS, OWNERS), 0, TGT_DEV // BLK)
    keeper = jax.random.randint(jax.random.fold_in(key, 12), (OWNERS, OWNERS), 0, 4) > 0
    diagonal = jnp.eye(OWNERS, dtype=bool)
    return jnp.where(keeper | diagonal, picked, -1).astype(jnp.int32)


def draw_source_blocks(key, part):
    return source_table(key)


def draw_tile_slot(key, part):
    table = source_table(key)
    tile_rows = NODES // BLK
    wanted = jax.random.randint(jax.random.fold_in(key, 13), (REL, tile_rows, SLOTS), 0, OWNERS)
    home = (jnp.arange(tile_rows, dtype=jnp.int32) // (TGT_DEV // BLK))[None, :, None]
    home_full = jnp.broadcast_to(home, (REL, tile_rows, SLOTS))
    listed = table[home_full, wanted] >= 0
    return jnp.where(listed, wanted, home_full).astype(jnp.int32)


def draw_tile_count(key, part):
    tile_rows = NODES // BLK
    hotness = jax.random.randint(jax.random.fold_in(key, 21), (REL, OWNERS), 0, 4) == 0
    hot_rows = jnp.repeat(hotness, TGT_DEV // BLK, axis=1)
    higher = jax.random.randint(jax.random.fold_in(key, 22), (REL, tile_rows), SLOTS // 2 + 1, SLOTS + 1)
    lower_counts = jax.random.randint(jax.random.fold_in(key, 23), (REL, tile_rows), 1, SLOTS // 2 + 1)
    counts = jnp.where(hot_rows, higher, lower_counts)
    forced = jnp.arange(tile_rows)[None, :] == jnp.arange(REL)[:, None] * 5 % tile_rows
    return jnp.where(forced, SLOTS, counts).astype(jnp.int32)


def draw_tile_values(key, part):
    shape_all = (REL, NODES, SLOTS, BLK)
    uniform_ints = jax.random.randint(jax.random.fold_in(key, 31), shape_all, 0, 15)
    levels = jnp.where(uniform_ints < 9, 0, (uniform_ints - 9) // 2 + 1)
    row_alive = jax.random.randint(jax.random.fold_in(key, 33), (REL, NODES, 1, 1), 0, 16) > 0
    return (levels * row_alive).astype(jnp.int32)


def level_of(key, shape, shards, least, largest):
    factor_of, own = 1.0, jax.random.fold_in(key, 6)
    for dim, blocks in shards:
        heights = jnp.exp(jax.random.uniform(jax.random.fold_in(own, dim), (blocks,), jnp.float32, least / len(shards), largest / len(shards)))
        factor_of = factor_of * jnp.repeat(heights, shape[dim] // blocks).reshape([-1 if axis == dim else 1 for axis in range(len(shape))])
    return factor_of


def centred(stream_key, extent, deviation, reach, split=(), kind=jnp.bfloat16):
    drawn = jax.random.normal(stream_key, extent, jnp.float32) * deviation
    if len(split) > 0:
        drawn = level_of(stream_key, extent, split, -0.22, 0.18) * drawn
    return jnp.clip(drawn, min=-reach, max=reach).astype(kind)


def setup_inputs(seed: int = 0) -> dict:
    key_list = jax.random.split(jax.random.key(seed), 9)
    features = centred(key_list[0], (NODES, D), 1.0, 6.0, ((0, 8),))
    weights = centred(key_list[1], (REL, D, D), (4 * D) ** -0.5, 0.109375, ((0, 4),))
    bias = centred(key_list[2], (D,), 0.5, 3.0, (), jnp.float32)
    cotangent = centred(key_list[3], (NODES, D), (8.0 / NODES ** 0.5), 1.0546875, ((0, 8),))
    tile_values = draw_tile_values(jax.random.fold_in(key_list[8], 71), 0)
    tile_count = draw_tile_count(jax.random.fold_in(key_list[8], 71), 0)
    tile_slot = draw_tile_slot(jax.random.fold_in(key_list[8], 71), 0)
    source_blocks = draw_source_blocks(jax.random.fold_in(key_list[8], 71), 0)
    return {"features": features, "weights": weights, "bias": bias, "cotangent": cotangent, "tile_values": tile_values, "tile_count": tile_count, "tile_slot": tile_slot, "source_blocks": source_blocks}


HIGHEST = lax.Precision.HIGHEST

def silu_pair(values):
    sigmoid = jax.nn.sigmoid(values)
    return (values * sigmoid, sigmoid * (1.0 + values * (1.0 - sigmoid)))

def reference(features, weights, bias, cotangent, tile_values, tile_count, tile_slot, source_blocks):
    sections = TGT_DEV // BLK
    own_blocks = features.reshape(OWNERS, sections, BLK, D)
    weights_wide = weights.astype(jnp.float32)
    owner_ids = jnp.arange(OWNERS, dtype=jnp.int32)
    section_ids = jnp.arange(sections, dtype=jnp.int32)
    slot_ids = jnp.arange(SLOTS, dtype=jnp.int32)

    def one_block(state_pair, target):
        weight_sum, feature_sum = state_pair
        values = lax.dynamic_slice_in_dim(tile_values, target * TGT_DEV, TGT_DEV, 1)
        counts = lax.dynamic_slice_in_dim(tile_count, target * sections, sections, 1)
        slots_here = lax.dynamic_slice_in_dim(tile_slot, target * sections, sections, 1)
        requested = lax.dynamic_index_in_dim(source_blocks, target, 0, keepdims=False)
        cot_rows = lax.dynamic_slice_in_dim(cotangent, target * TGT_DEV, TGT_DEV, 0)
        chosen = own_blocks[owner_ids, jnp.maximum(requested, 0)]
        fetched = jnp.where((requested >= 0)[:, None, None], chosen, jnp.zeros_like(chosen))
        live_mask = (slot_ids[None, None, :] < counts[:, :, None]).astype(jnp.int32)
        counted = values.reshape(REL, sections, BLK, SLOTS, BLK) * live_mask[:, :, None, :, None]
        degree = lax.optimization_barrier(jnp.sum(counted, axis=(3, 4))).astype(jnp.float32)
        adjacency = (counted.astype(jnp.float32) / jnp.sqrt(jnp.maximum(degree, 1.0))[..., None, None]).astype(jnp.bfloat16)
        adj_wide = adjacency.astype(jnp.float32)
        sources = fetched[slots_here].astype(jnp.float32)
        messages = jnp.einsum('rqisc,rqscd->rqid', adj_wide, sources, precision=HIGHEST).astype(jnp.bfloat16)
        msg_wide = messages.reshape(REL, TGT_DEV, D).astype(jnp.float32)
        preact = jnp.einsum('rnd,rde->ne', msg_wide, weights_wide, precision=HIGHEST) + bias
        activated, derivative = silu_pair(preact)
        grad_pre = (cot_rows.astype(jnp.float32) * derivative).astype(jnp.bfloat16)
        grad_wide = grad_pre.astype(jnp.float32)
        grad_messages = jnp.einsum('ne,rde->rnd', grad_wide, weights_wide, precision=HIGHEST).astype(jnp.bfloat16)
        weight_sum = weight_sum + jnp.einsum('rnd,ne->rde', msg_wide, grad_wide, precision=HIGHEST)
        grads_blocked = grad_messages.astype(jnp.float32).reshape(REL, sections, BLK, D)
        contrib = jnp.einsum('rqisc,rqid->rqscd', adj_wide, grads_blocked, precision=HIGHEST)
        selector = (slots_here[..., None] == owner_ids).astype(jnp.float32)
        grouped = jnp.einsum('grqso,grqscd->gocd', selector.reshape(N_REL, REL_DEV, sections, SLOTS, OWNERS), contrib.reshape(N_REL, REL_DEV, sections, SLOTS, BLK, D), precision=HIGHEST)
        rounded = lax.optimization_barrier(grouped.astype(jnp.bfloat16)).astype(jnp.float32)
        per_owner = lax.optimization_barrier(jnp.sum(rounded, axis=0))
        placed = (requested[:, None] == section_ids[None, :]).astype(jnp.float32)
        feature_sum = feature_sum + jnp.einsum('ok,ocd->okcd', placed, per_owner, precision=HIGHEST)
        return ((weight_sum, feature_sum), activated.astype(jnp.bfloat16))
    initial = (jnp.zeros((REL, D, D), jnp.float32), jnp.zeros((OWNERS, sections, BLK, D), jnp.float32))
    finals, outputs = lax.scan(one_block, initial, jnp.arange(OWNERS, dtype=jnp.int32))
    weight_sum, feature_sum = finals
    return (outputs.reshape(NODES, D), weight_sum, feature_sum.reshape(NODES // BLK, BLK, D))
```

```python
import functools

import jax
import jax.numpy as jnp
from jax import lax
from jax.experimental import pallas as pl
from jax.experimental.pallas import tpu as pltpu
from jax.sharding import PartitionSpec as P

MESH = pl.DeviceIdType.MESH
F32 = jnp.float32
BF16 = jnp.bfloat16


def aligned(start, size, multiple):
    return pl.ds(pl.multiple_of(start, multiple), size)


def is_one(condition):
    return condition.astype(jnp.int32).astype(F32)


def pack(value, first, width):
    half = value.shape[0] // 2
    return jnp.concatenate(
        [value[:half, first : first + width], value[half:, first : first + width]], axis=1
    )


def kernel(
    n, groups,
    table, counts, slots,
    feat, cot, bias, values_hbm, weights_hbm,
    out, grad_w, grad_f,
    weights, values, staged, fetched, adj, scale, msg, msg_t, pre,
    pre_send, pre_recv, gp_all, gp, gm,
    part, part_recv, part_sum, part_back,
    wg_pair, wg_pair_recv, wg_send, wg_recv,
    load_sem, a_send, a_recv, b_send, b_recv, p_send, p_recv, g_send, g_recv,
    d_send, d_recv, e_send, e_recv, w_send, w_recv, x_send, x_recv,
):
    me = lax.axis_index("tgt")
    grp = lax.axis_index("rel")
    rows, width = feat.shape
    relations = weights.shape[0]
    slot_total = slots.shape[2]
    blk = values.shape[1] // (rows * slot_total) * values.shape[2]
    sections = rows // blk
    quarter = blk // groups
    share = width // groups
    chips = n // 2
    chip, core = me // 2, lax.rem(me, 2)

    def tgt(j):
        return lax.rem(me + j, n)

    def tgt_back(j):
        return lax.rem(me + n - j, n)

    def rel(i):
        return lax.rem(grp + i, groups)

    load_w = pltpu.make_async_copy(weights_hbm, weights, load_sem.at[0])
    load_v = pltpu.make_async_copy(values_hbm, values, load_sem.at[1])
    load_v.start()
    load_w.start()

    barrier = pltpu.get_barrier_semaphore()

    @pl.loop(1, n)
    def _(j):
        pl.semaphore_signal(barrier, inc=1, device_id=(grp, tgt(j)), device_id_type=MESH)

    for i in range(1, groups):
        pl.semaphore_signal(barrier, inc=1, device_id=(rel(i), me), device_id_type=MESH)

    @pl.loop(0, n)
    def _(t):
        total = jnp.zeros((quarter, width), F32)
        for k in range(sections):
            block = feat[aligned(k * blk + grp * quarter, quarter, quarter), :].astype(F32)
            total = total + block * is_one(table[t, me] == k)
        staged[t] = total.astype(BF16)

    total = jnp.zeros((blk, width), F32)
    for k in range(sections):
        total = total + feat[k * blk : (k + 1) * blk, :].astype(F32) * is_one(table[me, me] == k)
    fetched[aligned(me * blk, blk, blk), :] = total.astype(BF16)
    pl.semaphore_wait(barrier, n - 1 + groups - 1)

    def fetch(j):
        return pltpu.make_async_remote_copy(
            src_ref=staged.at[tgt(j)],
            dst_ref=fetched.at[aligned(me * blk + grp * quarter, quarter, quarter), :],
            send_sem=a_send.at[j], recv_sem=a_recv.at[j],
            device_id=(grp, tgt(j)), device_id_type=MESH,
        )

    @pl.loop(1, n)
    def _(j):
        fetch(j).start()

    def spread(j, i):
        rows_at = aligned(tgt_back(j) * blk + grp * quarter, quarter, quarter)
        return pltpu.make_async_remote_copy(
            src_ref=fetched.at[rows_at, :], dst_ref=fetched.at[rows_at, :],
            send_sem=b_send.at[j, i], recv_sem=b_recv.at[j, i],
            device_id=(rel(i), me), device_id_type=MESH,
        )

    load_v.wait()

    @pl.loop(0, relations * sections)
    def _(b):
        r, q = b // sections, lax.rem(b, sections)
        count = counts[r, q]

        def tile(s):
            start = (q * blk * slot_total) + s
            live = (s < count).astype(jnp.int32)
            return values[r, pl.ds(start, blk, stride=slot_total), :] * live

        total = tile(0)
        for s in range(1, slot_total):
            total = total + tile(s)
        degree = jnp.sum(total.astype(F32), axis=1, keepdims=True)
        root = 1.0 / jnp.sqrt(jnp.maximum(degree, 1.0))
        scale[aligned(b * blk, blk, blk), :] = jnp.broadcast_to(root, (blk, 128))

        @pl.loop(0, n)
        def _(o):
            entry = jnp.zeros((blk, blk), jnp.int32)
            for s in range(slot_total):
                entry = entry + tile(s) * (slots[r, q, s] == o).astype(jnp.int32)
            adj[aligned(b * blk, blk, blk), aligned(o * blk, blk, blk)] = entry.astype(F32).astype(BF16)

    @pl.loop(1, n)
    def _(j):
        fetch(j).wait_recv()
        for i in range(1, groups):
            spread(j, i).start()

    load_w.wait()

    @pl.loop(1, n)
    def _(j):
        for i in range(1, groups):
            spread(j, i).wait_recv()

    for r in range(relations):
        @pl.loop(0, sections)
        def _(q):
            at = aligned(r * rows + q * blk, blk, blk)
            acc = jnp.dot(adj[at, :], fetched[...], preferred_element_type=F32)
            message = acc * scale[at, 0:1]
            msg[at, :] = message.astype(BF16)

    @pl.loop(0, sections)
    def _(q):
        total = None
        for r in range(relations):
            part_r = jnp.dot(
                msg[aligned(r * rows + q * blk, blk, blk), :], weights[r], preferred_element_type=F32
            )
            total = part_r if total is None else total + part_r
        pre[aligned(q * blk, blk, blk), :] = total

    whole = pre[...]
    for k in range(groups):
        pre_send[k] = pack(whole, k * share, share).astype(BF16)

    def reduce_pre(i):
        return pltpu.make_async_remote_copy(
            src_ref=pre_send.at[rel(i)], dst_ref=pre_recv.at[i],
            send_sem=p_send.at[i], recv_sem=p_recv.at[i],
            device_id=(rel(i), me), device_id_type=MESH,
        )

    for i in range(1, groups):
        reduce_pre(i).start()

    for r in range(relations):
        turned = msg[r * rows : (r + 1) * rows, :].astype(F32).T
        msg_t[r] = turned.reshape(n, width // n, rows).astype(BF16)

    total = pre_send[grp].astype(F32)
    for i in range(1, groups):
        reduce_pre(i).wait_recv()
        total = total + pre_recv[i].astype(F32)
    pre_act = total + bias[grp]
    sigmoid = jax.nn.sigmoid(pre_act)
    out[...] = (pre_act * sigmoid).astype(BF16)
    derivative = sigmoid * (1.0 + pre_act * (1.0 - sigmoid))
    for k in range(groups):
        @pl.when(grp == k)
        def _():
            piece = pack(cot[...].astype(F32), k * share, share)
            gp_all[k] = (piece * derivative).astype(BF16)

    def gather_gp(i):
        return pltpu.make_async_remote_copy(
            src_ref=gp_all.at[grp], dst_ref=gp_all.at[grp],
            send_sem=g_send.at[i], recv_sem=g_recv.at[i],
            device_id=(rel(i), me), device_id_type=MESH,
        )

    for i in range(1, groups):
        gather_gp(i).start()
    for i in range(1, groups):
        gather_gp(i).wait_recv()
    half = rows // 2
    for h in range(2):
        gp[h * half : (h + 1) * half, :] = jnp.concatenate(
            [gp_all[k][:, h * share : (h + 1) * share].astype(F32) for k in range(groups)], axis=1
        ).astype(BF16)

    def weight_chunk(r, t):
        return jnp.dot(msg_t[r, t], gp[...], preferred_element_type=F32)

    def pair(z):
        return pltpu.make_async_remote_copy(
            src_ref=wg_pair.at[z], dst_ref=wg_pair_recv.at[z],
            send_sem=w_send.at[z], recv_sem=w_recv.at[z],
            device_id=(grp, chip * 2 + 1 - core), device_id_type=MESH,
        )

    @pl.loop(0, chips)
    def _(z):
        for r in range(relations):
            wg_pair[z, r] = weight_chunk(r, z * 2 + 1 - core).astype(BF16)
        pair(z).start()

    def cross(j):
        z = lax.rem(chip + j, chips)
        return pltpu.make_async_remote_copy(
            src_ref=wg_send.at[j], dst_ref=wg_recv.at[j],
            send_sem=x_send.at[j], recv_sem=x_recv.at[j],
            device_id=(grp, z * 2 + core), device_id_type=MESH,
        )

    @pl.loop(0, chips)
    def _(z):
        pair(z).wait_recv()

    @pl.loop(1, chips)
    def _(j):
        z = lax.rem(chip + j, chips)
        for r in range(relations):
            summed = weight_chunk(r, z * 2 + core) + wg_pair_recv[z, r].astype(F32)
            wg_send[j, r] = summed.astype(BF16)
        cross(j).start()

    for r in range(relations):
        grad_w[r] = weight_chunk(r, me) + wg_pair_recv[chip, r].astype(F32)

    for r in range(relations):
        @pl.loop(0, sections)
        def _(q):
            at = aligned(r * rows + q * blk, blk, blk)
            grads = lax.dot_general(
                gp[aligned(q * blk, blk, blk), :], weights[r],
                (((1,), (1,)), ((), ())), preferred_element_type=F32,
            )
            gm[at, :] = (grads * scale[at, 0:1]).astype(BF16)

    def reduce_part(o, i):
        return pltpu.make_async_remote_copy(
            src_ref=part.at[o, aligned(rel(i) * quarter, quarter, quarter), :],
            dst_ref=part_recv.at[i, o],
            send_sem=d_send.at[o, i], recv_sem=d_recv.at[o, i],
            device_id=(rel(i), me), device_id_type=MESH,
        )

    @pl.loop(0, n)
    def _(j):
        o = tgt(j)
        block = lax.dot_general(
            adj[:, aligned(o * blk, blk, blk)], gm[...],
            (((0,), (0,)), ((), ())), preferred_element_type=F32,
        )
        part[o] = block.astype(BF16)
        for i in range(1, groups):
            reduce_part(o, i).start()

    def give_back(j):
        return pltpu.make_async_remote_copy(
            src_ref=part_sum.at[tgt(j)], dst_ref=part_back.at[me],
            send_sem=e_send.at[j], recv_sem=e_recv.at[j],
            device_id=(grp, tgt(j)), device_id_type=MESH,
        )

    def reduced(o):
        total = part[o, aligned(grp * quarter, quarter, quarter), :].astype(F32)
        for i in range(1, groups):
            reduce_part(o, i).wait_recv()
            total = total + part_recv[i, o].astype(F32)
        return total.astype(BF16)

    part_back[me] = reduced(me)

    @pl.loop(1, n)
    def _(j):
        part_sum[tgt(j)] = reduced(tgt(j))
        give_back(j).start()

    @pl.loop(1, chips)
    def _(j):
        cross(j).wait_recv()
        for r in range(relations):
            grad_w[r] = grad_w[r] + wg_recv[j, r].astype(F32)

    @pl.loop(1, n)
    def _(j):
        give_back(j).wait_recv()

    for k in range(sections):
        grad_f[k] = jnp.zeros((quarter, width), F32)

    @pl.loop(0, n)
    def _(t):
        wanted = table[t, me]
        addend = part_back[t].astype(F32)
        for k in range(sections):
            grad_f[k] = grad_f[k] + addend * is_one(wanted == k)

    @pl.loop(1, n)
    def _(j):
        fetch(j).wait_send()
        give_back(j).wait_send()
        for i in range(1, groups):
            spread(j, i).wait_send()

    for i in range(1, groups):
        reduce_pre(i).wait_send()
        gather_gp(i).wait_send()

    @pl.loop(0, n)
    def _(o):
        for i in range(1, groups):
            reduce_part(o, i).wait_send()

    @pl.loop(0, chips)
    def _(z):
        pair(z).wait_send()

    @pl.loop(1, chips)
    def _(j):
        cross(j).wait_send()


def per_device(
    n, groups,
    features, weights, bias, cotangent, tile_values, tile_count, tile_slot, source_blocks,
):
    rows, width = features.shape
    relations, _, slot_total, blk = tile_values.shape
    sections = rows // blk
    quarter, share, chunk, chips = blk // groups, width // groups, width // n, n // 2
    half = rows // 2
    bias_packed = jnp.tile(bias.reshape(groups, 1, share), (1, 1, 2))
    vmem = pl.BlockSpec(memory_space=pltpu.VMEM)
    smem = pl.BlockSpec(memory_space=pltpu.SMEM)
    anywhere = pl.BlockSpec(memory_space=pl.ANY)
    dma = pltpu.SemaphoreType.DMA
    out, grad_w, grad_f = pl.pallas_call(
        functools.partial(kernel, n, groups),
        out_shape=(
            jax.ShapeDtypeStruct((half, 2 * share), BF16),
            jax.ShapeDtypeStruct((relations, chunk, width), F32),
            jax.ShapeDtypeStruct((sections, quarter, width), F32),
        ),
        in_specs=[smem, smem, smem, vmem, vmem, vmem, anywhere, anywhere],
        out_specs=(vmem, vmem, vmem),
        scratch_shapes=[
            pltpu.VMEM((relations, width, width), BF16),
            pltpu.VMEM((relations, rows * slot_total, blk), jnp.int32),
            pltpu.VMEM((n, quarter, width), BF16),
            pltpu.VMEM((n * blk, width), BF16),
            pltpu.VMEM((relations * rows, n * blk), BF16),
            pltpu.VMEM((relations * rows, 128), F32),
            pltpu.VMEM((relations * rows, width), BF16),
            pltpu.VMEM((relations, n, chunk, rows), BF16),
            pltpu.VMEM((rows, width), F32),
            pltpu.VMEM((groups, half, 2 * share), BF16),
            pltpu.VMEM((groups, half, 2 * share), BF16),
            pltpu.VMEM((groups, half, 2 * share), BF16),
            pltpu.VMEM((rows, width), BF16),
            pltpu.VMEM((relations * rows, width), BF16),
            pltpu.VMEM((n, blk, width), BF16),
            pltpu.VMEM((groups, n, quarter, width), BF16),
            pltpu.VMEM((n, quarter, width), BF16),
            pltpu.VMEM((n, quarter, width), BF16),
            pltpu.VMEM((chips, relations, chunk, width), BF16),
            pltpu.VMEM((chips, relations, chunk, width), BF16),
            pltpu.VMEM((chips, relations, chunk, width), BF16),
            pltpu.VMEM((chips, relations, chunk, width), BF16),
            dma((2,)),
            dma((n,)), dma((n,)),
            dma((n, groups)), dma((n, groups)),
            dma((groups,)), dma((groups,)),
            dma((groups,)), dma((groups,)),
            dma((n, groups)), dma((n, groups)),
            dma((n,)), dma((n,)),
            dma((chips,)), dma((chips,)),
            dma((chips,)), dma((chips,)),
        ],
        compiler_params=pltpu.CompilerParams(
            collective_id=0, has_side_effects=True, vmem_limit_bytes=60 << 20
        ),
        name="layer",
    )(
        source_blocks, tile_count, tile_slot,
        features, cotangent, bias_packed,
        tile_values.reshape(relations, rows * slot_total, blk), weights,
    )
    output = out.reshape(half, 2, share).swapaxes(0, 1).reshape(rows, share)
    return (output, grad_w, grad_f)


def solution(mesh):
    placed = (
        P("tgt", None),
        P("rel", None, None),
        P(),
        P("tgt", None),
        P("rel", "tgt", None, None),
        P("rel", "tgt"),
        P("rel", "tgt", None),
        P(),
    )
    return jax.shard_map(
        functools.partial(per_device, mesh.shape["tgt"], mesh.shape["rel"]),
        mesh=mesh,
        in_specs=placed,
        out_specs=(P("tgt", "rel"), P("rel", "tgt", None), P("tgt", "rel", None)),
        check_vma=False,
    )
```

```python
import functools

import jax
import jax.numpy as jnp
from jax import lax
from jax.experimental import pallas as pl
from jax.experimental.pallas import tpu as pltpu
from jax.sharding import PartitionSpec as P

MESH = pl.DeviceIdType.MESH
F32 = jnp.float32
BF16 = jnp.bfloat16


def aligned(start, size, multiple):
    return pl.ds(pl.multiple_of(start, multiple), size)


def is_one(condition):
    return condition.astype(jnp.int32).astype(F32)


def pack(value, first, width):
    half = value.shape[0] // 2
    return jnp.concatenate(
        [value[:half, first : first + width], value[half:, first : first + width]], axis=1
    )


def kernel(
    n, groups,
    table, counts, slots,
    feat, cot, bias, values_hbm, weights_hbm,
    out, grad_w, grad_f,
    weights, values, staged, partner_staged, masked, fetched, adj, scale, msg, msg_t, pre,
    pre_send, pre_recv, cot_own, bias_own, gp_all, gp, gm,
    part, part_recv, part_sum, part_back,
    wg_pair, wg_pair_recv, up_send, up_recv, down_send, down_recv,
    load_sem, a_send, a_recv, b_send, b_recv, p_send, p_recv, g_send, g_recv,
    d_send, d_recv, e_send, e_recv, w_send, w_recv, u_send, u_recv, v_send, v_recv,
):
    me = lax.axis_index("tgt")
    grp = lax.axis_index("rel")
    rows, width = feat.shape
    relations = weights.shape[0]
    slot_total = slots.shape[2]
    blk = values.shape[1] // (rows * slot_total) * values.shape[2]
    sections = rows // blk
    quarter = blk // groups
    share = width // groups
    chips = n // 2
    chip, core = me // 2, lax.rem(me, 2)

    def tgt(j):
        return lax.rem(chip + j // 2, chips) * 2 + lax.rem(core + lax.rem(j, 2), 2)

    def tgt_back(j):
        return lax.rem(chip + chips - j // 2, chips) * 2 + lax.rem(core + lax.rem(j, 2), 2)

    partner = chip * 2 + 1 - core
    row, column = grp // 2, lax.rem(grp, 2)
    beside = row * 2 + 1 - column
    above = (1 - row) * 2 + column

    def rel(i):
        return lax.rem(grp + i, groups)

    load_w = pltpu.make_async_copy(weights_hbm, weights, load_sem.at[0])
    load_v = pltpu.make_async_copy(values_hbm, values, load_sem.at[1])
    load_v.start()
    load_w.start()

    barrier = pltpu.get_barrier_semaphore()

    @pl.loop(1, n)
    def _(j):
        pl.semaphore_signal(barrier, inc=1, device_id=(grp, tgt(j)), device_id_type=MESH)

    for i in range(1, groups):
        pl.semaphore_signal(barrier, inc=1, device_id=(rel(i), me), device_id_type=MESH)

    @pl.loop(0, n)
    def _(t):
        total = jnp.zeros((quarter, width), F32)
        for k in range(sections):
            block = feat[aligned(k * blk + grp * quarter, quarter, quarter), :].astype(F32)
            total = total + block * is_one(table[t, me] == k)
        staged[t] = total.astype(BF16)

    def whole_block(t):
        total = jnp.zeros((blk, width), F32)
        for k in range(sections):
            total = total + feat[k * blk : (k + 1) * blk, :].astype(F32) * is_one(table[t, me] == k)
        return total.astype(BF16)

    fetched[aligned(me * blk, blk, blk), :] = whole_block(me)
    partner_staged[...] = whole_block(partner)
    pl.semaphore_wait(barrier, n - 1 + groups - 1)

    def fetch(j):
        return pltpu.make_async_remote_copy(
            src_ref=staged.at[tgt(j)],
            dst_ref=fetched.at[aligned(me * blk + grp * quarter, quarter, quarter), :],
            send_sem=a_send.at[j], recv_sem=a_recv.at[j],
            device_id=(grp, tgt(j)), device_id_type=MESH,
        )

    fetch_pair = pltpu.make_async_remote_copy(
        src_ref=partner_staged, dst_ref=fetched.at[aligned(me * blk, blk, blk), :],
        send_sem=a_send.at[1], recv_sem=a_recv.at[1],
        device_id=(grp, partner), device_id_type=MESH,
    )

    @pl.loop(2, n)
    def _(j):
        fetch(j).start()

    fetch_pair.start()

    def spread(j, way):
        size = quarter if way < 2 else quarter // 2
        source = (grp, grp, beside, above)[way]
        extra = quarter // 2 if way == 3 else 0
        peer = (beside, above, above, beside)[way]
        rows_at = aligned(tgt_back(j) * blk + source * quarter + extra, size, size)
        return pltpu.make_async_remote_copy(
            src_ref=fetched.at[rows_at, :], dst_ref=fetched.at[rows_at, :],
            send_sem=b_send.at[j, way], recv_sem=b_recv.at[j, way],
            device_id=(peer, me), device_id_type=MESH,
        )

    def pass_on(j):
        spread(j, 0).wait_recv()
        spread(j, 2).start()
        spread(j, 1).wait_recv()
        spread(j, 3).start()

    load_v.wait()

    @pl.loop(0, relations * sections)
    def _(b):
        r, q = b // sections, lax.rem(b, sections)
        count = counts[r, q]

        def tile(s):
            start = (q * blk * slot_total) + s
            live = (s < count).astype(jnp.int32)
            return values[r, pl.ds(start, blk, stride=slot_total), :] * live

        total = jnp.zeros((blk, blk), jnp.int32)
        for s in range(slot_total):
            live_tile = tile(s)
            masked[s] = live_tile
            total = total + live_tile
        degree = jnp.sum(total.astype(F32), axis=1, keepdims=True)
        root = 1.0 / jnp.sqrt(jnp.maximum(degree, 1.0))
        scale[aligned(b * blk, blk, blk), :] = jnp.broadcast_to(root, (blk, 128))

        @pl.loop(0, n)
        def _(o):
            entry = jnp.zeros((blk, blk), jnp.int32)
            for s in range(slot_total):
                entry = entry + masked[s] * (slots[r, q, s] == o).astype(jnp.int32)
            adj[aligned(b * blk, blk, blk), aligned(o * blk, blk, blk)] = entry.astype(F32).astype(BF16)

    @pl.loop(2, n)
    def _(j):
        fetch(j).wait_recv()
        spread(j, 0).start()
        spread(j, 1).start()

        @pl.when(j > 2)
        def _():
            pass_on(j - 1)

    pass_on(n - 1)
    load_w.wait()
    fetch_pair.wait_recv()

    @pl.loop(2, n)
    def _(j):
        spread(j, 2).wait_recv()
        spread(j, 3).wait_recv()

    for r in range(relations):
        @pl.loop(0, sections)
        def _(q):
            at = aligned(r * rows + q * blk, blk, blk)
            acc = jnp.dot(adj[at, :], fetched[...], preferred_element_type=F32)
            message = acc * scale[at, 0:1]
            msg[at, :] = message.astype(BF16)

    @pl.loop(0, sections)
    def _(q):
        total = None
        for r in range(relations):
            part_r = jnp.dot(
                msg[aligned(r * rows + q * blk, blk, blk), :], weights[r], preferred_element_type=F32
            )
            total = part_r if total is None else total + part_r
        pre[aligned(q * blk, blk, blk), :] = total

    whole = pre[...]
    for k in range(groups):
        pre_send[k] = pack(whole, k * share, share).astype(BF16)

    piece_rows = rows // 4

    def reduce_pre(i, p):
        at = slice(p * piece_rows, (p + 1) * piece_rows)
        return pltpu.make_async_remote_copy(
            src_ref=pre_send.at[rel(i), at, :], dst_ref=pre_recv.at[i, at, :],
            send_sem=p_send.at[i, p], recv_sem=p_recv.at[i, p],
            device_id=(rel(i), me), device_id_type=MESH,
        )

    for p in range(2):
        for i in range(1, groups):
            reduce_pre(i, p).start()

    for r in range(relations):
        turned = msg[r * rows : (r + 1) * rows, :].astype(F32).T
        msg_t[r] = turned.reshape(n, width // n, rows).astype(BF16)

    for k in range(groups):
        @pl.when(grp == k)
        def _():
            cot_own[...] = pack(cot[...].astype(F32), k * share, share)
            piece = bias[:, k * share : (k + 1) * share]
            bias_own[...] = jnp.concatenate([piece, piece], axis=1)

    def gather_gp(i, p):
        at = slice(p * piece_rows, (p + 1) * piece_rows)
        return pltpu.make_async_remote_copy(
            src_ref=gp_all.at[grp, at, :], dst_ref=gp_all.at[grp, at, :],
            send_sem=g_send.at[i, p], recv_sem=g_recv.at[i, p],
            device_id=(rel(i), me), device_id_type=MESH,
        )

    for p in range(2):
        at = slice(p * piece_rows, (p + 1) * piece_rows)
        total = pre_send[grp, at, :].astype(F32)
        for i in range(1, groups):
            reduce_pre(i, p).wait_recv()
            total = total + pre_recv[i, at, :].astype(F32)
        pre_act = total + bias_own[...]
        sigmoid = jax.nn.sigmoid(pre_act)
        derivative = sigmoid * (1.0 + pre_act * (1.0 - sigmoid))
        gp_all[grp, at, :] = (cot_own[at, :] * derivative).astype(BF16)
        for i in range(1, groups):
            gather_gp(i, p).start()
        out[at, :] = (pre_act * sigmoid).astype(BF16)

    for p in range(2):
        for i in range(1, groups):
            gather_gp(i, p).wait_recv()
    half = rows // 2
    for h in range(2):
        gp[h * half : (h + 1) * half, :] = jnp.concatenate(
            [gp_all[k][:, h * share : (h + 1) * share].astype(F32) for k in range(groups)], axis=1
        ).astype(BF16)

    def weight_chunk(r, t):
        return jnp.dot(msg_t[r, t], gp[...], preferred_element_type=F32)

    def pair(z):
        return pltpu.make_async_remote_copy(
            src_ref=wg_pair.at[z], dst_ref=wg_pair_recv.at[z],
            send_sem=w_send.at[z], recv_sem=w_recv.at[z],
            device_id=(grp, partner), device_id_type=MESH,
        )

    @pl.loop(0, chips)
    def _(z):
        for r in range(relations):
            wg_pair[z, r] = weight_chunk(r, z * 2 + 1 - core).astype(BF16)
        pair(z).start()

    def climb(d):
        return pltpu.make_async_remote_copy(
            src_ref=up_send.at[d], dst_ref=up_recv.at[d],
            send_sem=u_send.at[d], recv_sem=u_recv.at[d],
            device_id=(grp, jnp.minimum(chip + 1, chips - 1) * 2 + core), device_id_type=MESH,
        )

    def descend(d):
        return pltpu.make_async_remote_copy(
            src_ref=down_send.at[d], dst_ref=down_recv.at[d],
            send_sem=v_send.at[d], recv_sem=v_recv.at[d],
            device_id=(grp, jnp.maximum(chip - 1, 0) * 2 + core), device_id_type=MESH,
        )

    def chip_sum(r, z):
        return weight_chunk(r, z * 2 + core) + wg_pair_recv[z, r].astype(F32)

    def line_step(step):
        @pl.when(step >= chip)
        def _():
            d = chips - 1 - step + chip

            @pl.when(chip > 0)
            def _():
                climb(d).wait_recv()
                for r in range(relations):
                    up_send[d, r] = (chip_sum(r, d) + up_recv[d, r].astype(F32)).astype(BF16)

            @pl.when(chip == 0)
            def _():
                for r in range(relations):
                    up_send[d, r] = chip_sum(r, d).astype(BF16)

            climb(d).start()

        @pl.when(step >= chips - 1 - chip)
        def _():
            d = step - chips + 1 + chip

            @pl.when(chip < chips - 1)
            def _():
                descend(d).wait_recv()
                for r in range(relations):
                    down_send[d, r] = (chip_sum(r, d) + down_recv[d, r].astype(F32)).astype(BF16)

            @pl.when(chip == chips - 1)
            def _():
                for r in range(relations):
                    down_send[d, r] = chip_sum(r, d).astype(BF16)

            descend(d).start()

    @pl.loop(0, chips)
    def _(z):
        pair(z).wait_recv()

    line_step(0)

    for r in range(relations):
        @pl.loop(0, sections)
        def _(q):
            at = aligned(r * rows + q * blk, blk, blk)
            grads = lax.dot_general(
                gp[aligned(q * blk, blk, blk), :], weights[r],
                (((1,), (1,)), ((), ())), preferred_element_type=F32,
            )
            gm[at, :] = (grads * scale[at, 0:1]).astype(BF16)

    def reduce_part(o, i):
        return pltpu.make_async_remote_copy(
            src_ref=part.at[o, aligned(rel(i) * quarter, quarter, quarter), :],
            dst_ref=part_recv.at[i, o],
            send_sem=d_send.at[o, i], recv_sem=d_recv.at[o, i],
            device_id=(rel(i), me), device_id_type=MESH,
        )

    @pl.loop(0, n)
    def _(j):
        o = tgt(j)
        block = lax.dot_general(
            adj[:, aligned(o * blk, blk, blk)], gm[...],
            (((0,), (0,)), ((), ())), preferred_element_type=F32,
        )
        part[o] = block.astype(BF16)
        for i in range(1, groups):
            reduce_part(o, i).start()

    @pl.loop(1, chips - 1)
    def _(step):
        line_step(step)

    for r in range(relations):
        grad_w[r] = chip_sum(r, chip)

    def give_back(j):
        return pltpu.make_async_remote_copy(
            src_ref=part_sum.at[tgt(j)], dst_ref=part_back.at[me],
            send_sem=e_send.at[j], recv_sem=e_recv.at[j],
            device_id=(grp, tgt(j)), device_id_type=MESH,
        )

    def reduced(o):
        total = part[o, aligned(grp * quarter, quarter, quarter), :].astype(F32)
        for i in range(1, groups):
            reduce_part(o, i).wait_recv()
            total = total + part_recv[i, o].astype(F32)
        return total.astype(BF16)

    part_back[me] = reduced(me)

    @pl.loop(1, n)
    def _(j):
        part_sum[tgt(j)] = reduced(tgt(j))
        give_back(j).start()

    @pl.when(chip > 0)
    def _():
        climb(chip).wait_recv()
        for r in range(relations):
            grad_w[r] = grad_w[r] + up_recv[chip, r].astype(F32)

    @pl.when(chip < chips - 1)
    def _():
        descend(chip).wait_recv()
        for r in range(relations):
            grad_w[r] = grad_w[r] + down_recv[chip, r].astype(F32)

    @pl.loop(1, n)
    def _(j):
        give_back(j).wait_recv()

    for k in range(sections):
        grad_f[k] = jnp.zeros((quarter, width), F32)

    @pl.loop(0, n)
    def _(t):
        wanted = table[t, me]
        addend = part_back[t].astype(F32)
        for k in range(sections):
            grad_f[k] = grad_f[k] + addend * is_one(wanted == k)

    fetch_pair.wait_send()

    @pl.loop(2, n)
    def _(j):
        fetch(j).wait_send()
        for way in range(4):
            spread(j, way).wait_send()

    @pl.loop(1, n)
    def _(j):
        give_back(j).wait_send()

    for i in range(1, groups):
        for p in range(2):
            reduce_pre(i, p).wait_send()
            gather_gp(i, p).wait_send()

    @pl.loop(0, n)
    def _(o):
        for i in range(1, groups):
            reduce_part(o, i).wait_send()

    @pl.loop(0, chips)
    def _(z):
        pair(z).wait_send()

        @pl.when(z > chip)
        def _():
            climb(z).wait_send()

        @pl.when(z < chip)
        def _():
            descend(z).wait_send()


def per_device(
    n, groups,
    features, weights, bias, cotangent, tile_values, tile_count, tile_slot, source_blocks,
):
    rows, width = features.shape
    relations, _, slot_total, blk = tile_values.shape
    sections = rows // blk
    quarter, share, chunk, chips = blk // groups, width // groups, width // n, n // 2
    half = rows // 2
    vmem = pl.BlockSpec(memory_space=pltpu.VMEM)
    smem = pl.BlockSpec(memory_space=pltpu.SMEM)
    anywhere = pl.BlockSpec(memory_space=pl.ANY)
    dma = pltpu.SemaphoreType.DMA
    out, grad_w, grad_f = pl.pallas_call(
        functools.partial(kernel, n, groups),
        out_shape=(
            jax.ShapeDtypeStruct((half, 2 * share), BF16),
            jax.ShapeDtypeStruct((relations, chunk, width), F32),
            jax.ShapeDtypeStruct((sections, quarter, width), F32),
        ),
        in_specs=[smem, smem, smem, vmem, vmem, vmem, anywhere, anywhere],
        out_specs=(vmem, vmem, vmem),
        scratch_shapes=[
            pltpu.VMEM((relations, width, width), BF16),
            pltpu.VMEM((relations, rows * slot_total, blk), jnp.int32),
            pltpu.VMEM((n, quarter, width), BF16),
            pltpu.VMEM((blk, width), BF16),
            pltpu.VMEM((slot_total, blk, blk), jnp.int32),
            pltpu.VMEM((n * blk, width), BF16),
            pltpu.VMEM((relations * rows, n * blk), BF16),
            pltpu.VMEM((relations * rows, 128), F32),
            pltpu.VMEM((relations * rows, width), BF16),
            pltpu.VMEM((relations, n, chunk, rows), BF16),
            pltpu.VMEM((rows, width), F32),
            pltpu.VMEM((groups, half, 2 * share), BF16),
            pltpu.VMEM((groups, half, 2 * share), BF16),
            pltpu.VMEM((half, 2 * share), F32),
            pltpu.VMEM((1, 2 * share), F32),
            pltpu.VMEM((groups, half, 2 * share), BF16),
            pltpu.VMEM((rows, width), BF16),
            pltpu.VMEM((relations * rows, width), BF16),
            pltpu.VMEM((n, blk, width), BF16),
            pltpu.VMEM((groups, n, quarter, width), BF16),
            pltpu.VMEM((n, quarter, width), BF16),
            pltpu.VMEM((n, quarter, width), BF16),
            pltpu.VMEM((chips, relations, chunk, width), BF16),
            pltpu.VMEM((chips, relations, chunk, width), BF16),
            pltpu.VMEM((chips, relations, chunk, width), BF16),
            pltpu.VMEM((chips, relations, chunk, width), BF16),
            pltpu.VMEM((chips, relations, chunk, width), BF16),
            pltpu.VMEM((chips, relations, chunk, width), BF16),
            dma((2,)),
            dma((n,)), dma((n,)),
            dma((n, 4)), dma((n, 4)),
            dma((groups, 2)), dma((groups, 2)),
            dma((groups, 2)), dma((groups, 2)),
            dma((n, groups)), dma((n, groups)),
            dma((n,)), dma((n,)),
            dma((chips,)), dma((chips,)),
            dma((chips,)), dma((chips,)),
            dma((chips,)), dma((chips,)),
        ],
        compiler_params=pltpu.CompilerParams(
            collective_id=0, has_side_effects=True, vmem_limit_bytes=60 << 20
        ),
        name="layer",
    )(
        source_blocks, tile_count, tile_slot,
        features, cotangent, bias.reshape(1, width),
        tile_values.reshape(relations, rows * slot_total, blk), weights,
    )
    output = out.reshape(half, 2, share).swapaxes(0, 1).reshape(rows, share)
    return (output, grad_w, grad_f)


def solution(mesh):
    placed = (
        P("tgt", None),
        P("rel", None, None),
        P(),
        P("tgt", None),
        P("rel", "tgt", None, None),
        P("rel", "tgt"),
        P("rel", "tgt", None),
        P(),
    )
    return jax.shard_map(
        functools.partial(per_device, mesh.shape["tgt"], mesh.shape["rel"]),
        mesh=mesh,
        in_specs=placed,
        out_specs=(P("tgt", "rel"), P("rel", "tgt", None), P("tgt", "rel", None)),
        check_vma=False,
    )
```

```python
import functools

import jax
import jax.numpy as jnp
from jax import lax
from jax.experimental import pallas as pl
from jax.experimental.pallas import tpu as pltpu
from jax.sharding import PartitionSpec as P

MESH = pl.DeviceIdType.MESH
F32 = jnp.float32
BF16 = jnp.bfloat16


def aligned(start, size, multiple):
    return pl.ds(pl.multiple_of(start, multiple), size)


def is_one(condition):
    return condition.astype(jnp.int32).astype(F32)


def pack(value, first, width):
    half = value.shape[0] // 2
    return jnp.concatenate(
        [value[:half, first : first + width], value[half:, first : first + width]], axis=1
    )


def kernel(
    n, groups,
    table, counts, slots,
    feat, cot, bias, values_hbm, weights_hbm,
    out, grad_w, grad_f,
    weights, values, staged, partner_staged, masked, fetched, adj, scale, msg, msg_t, wg_own, adj_t, pre,
    pre_send, pre_recv, cot_own, bias_own, gp_all, gp, gm,
    part, part_recv, part_sum, part_back,
    wg_pair, wg_pair_recv, up_send, up_recv, down_send, down_recv,
    load_sem, a_send, a_recv, b_send, b_recv, p_send, p_recv, g_send, g_recv,
    d_send, d_recv, e_send, e_recv, w_send, w_recv, u_send, u_recv, v_send, v_recv,
):
    me = lax.axis_index("tgt")
    grp = lax.axis_index("rel")
    rows, width = feat.shape
    relations = weights.shape[0]
    slot_total = slots.shape[2]
    blk = values.shape[1] // (rows * slot_total) * values.shape[2]
    sections = rows // blk
    quarter = blk // groups
    share = width // groups
    chips = n // 2
    chip, core = me // 2, lax.rem(me, 2)

    def tgt(j):
        return lax.rem(chip + j // 2, chips) * 2 + lax.rem(core + lax.rem(j, 2), 2)

    def tgt_back(j):
        return lax.rem(chip + chips - j // 2, chips) * 2 + lax.rem(core + lax.rem(j, 2), 2)

    partner = chip * 2 + 1 - core
    row, column = grp // 2, lax.rem(grp, 2)
    beside = row * 2 + 1 - column
    above = (1 - row) * 2 + column

    def rel(i):
        return lax.rem(grp + i, groups)

    load_w = pltpu.make_async_copy(weights_hbm, weights, load_sem.at[0])
    load_v = pltpu.make_async_copy(values_hbm, values, load_sem.at[1])
    load_v.start()
    load_w.start()

    barrier = pltpu.get_barrier_semaphore()

    @pl.loop(1, n)
    def _(j):
        pl.semaphore_signal(barrier, inc=1, device_id=(grp, tgt(j)), device_id_type=MESH)

    for i in range(1, groups):
        pl.semaphore_signal(barrier, inc=1, device_id=(rel(i), me), device_id_type=MESH)

    @pl.loop(0, n)
    def _(t):
        total = jnp.zeros((quarter, width), F32)
        for k in range(sections):
            block = feat[aligned(k * blk + grp * quarter, quarter, quarter), :].astype(F32)
            total = total + block * is_one(table[t, me] == k)
        staged[t] = total.astype(BF16)

    def whole_block(t):
        total = jnp.zeros((blk, width), F32)
        for k in range(sections):
            total = total + feat[k * blk : (k + 1) * blk, :].astype(F32) * is_one(table[t, me] == k)
        return total.astype(BF16)

    fetched[aligned(me * blk, blk, blk), :] = whole_block(me)
    partner_staged[...] = whole_block(partner)
    pl.semaphore_wait(barrier, n - 1 + groups - 1)

    def fetch(j):
        return pltpu.make_async_remote_copy(
            src_ref=staged.at[tgt(j)],
            dst_ref=fetched.at[aligned(me * blk + grp * quarter, quarter, quarter), :],
            send_sem=a_send.at[j], recv_sem=a_recv.at[j],
            device_id=(grp, tgt(j)), device_id_type=MESH,
        )

    fetch_pair = pltpu.make_async_remote_copy(
        src_ref=partner_staged, dst_ref=fetched.at[aligned(me * blk, blk, blk), :],
        send_sem=a_send.at[1], recv_sem=a_recv.at[1],
        device_id=(grp, partner), device_id_type=MESH,
    )

    @pl.loop(2, n)
    def _(j):
        fetch(j).start()

    fetch_pair.start()

    def spread(j, way):
        size = quarter if way < 2 else quarter // 2
        source = (grp, grp, beside, above)[way]
        extra = quarter // 2 if way == 3 else 0
        peer = (beside, above, above, beside)[way]
        rows_at = aligned(tgt_back(j) * blk + source * quarter + extra, size, size)
        return pltpu.make_async_remote_copy(
            src_ref=fetched.at[rows_at, :], dst_ref=fetched.at[rows_at, :],
            send_sem=b_send.at[j, way], recv_sem=b_recv.at[j, way],
            device_id=(peer, me), device_id_type=MESH,
        )

    def pass_on(j):
        spread(j, 0).wait_recv()
        spread(j, 2).start()
        spread(j, 1).wait_recv()
        spread(j, 3).start()

    def arrive(j):
        fetch(j).wait_recv()
        spread(j, 0).start()
        spread(j, 1).start()

    load_v.wait()

    @pl.loop(0, relations * sections)
    def _(b):
        r, q = b // sections, lax.rem(b, sections)
        count = counts[r, q]

        def tile(s):
            start = (q * blk * slot_total) + s
            live = (s < count).astype(jnp.int32)
            return values[r, pl.ds(start, blk, stride=slot_total), :] * live

        total = jnp.zeros((blk, blk), jnp.int32)
        for s in range(slot_total):
            live_tile = tile(s)
            masked[s] = live_tile
            total = total + live_tile
        degree = jnp.sum(total.astype(F32), axis=1, keepdims=True)
        root = 1.0 / jnp.sqrt(jnp.maximum(degree, 1.0))
        scale[aligned(b * blk, blk, blk), :] = jnp.broadcast_to(root, (blk, 128))

        @pl.loop(0, n)
        def _(o):
            entry = jnp.zeros((blk, blk), jnp.int32)
            for s in range(slot_total):
                entry = entry + masked[s] * (slots[r, q, s] == o).astype(jnp.int32)
            wide = entry.astype(F32)
            adj[aligned(b * blk, blk, blk), aligned(o * blk, blk, blk)] = wide.astype(BF16)
            adj_t[aligned(o * blk, blk, blk), aligned(b * blk, blk, blk)] = wide.T.astype(BF16)

        arrive(b + 2)

    @pl.loop(relations * sections + 2, n)
    def _(j):
        arrive(j)
        pass_on(j - relations * sections)

    @pl.loop(n - relations * sections, n)
    def _(j):
        pass_on(j)

    load_w.wait()
    fetch_pair.wait_recv()

    @pl.loop(2, n)
    def _(j):
        spread(j, 2).wait_recv()
        spread(j, 3).wait_recv()

    tile_width = 256

    @pl.loop(0, width // tile_width)
    def _(c):
        at = aligned(c * tile_width, tile_width, tile_width)
        acc = jnp.dot(adj[...], fetched[:, at], preferred_element_type=F32)
        msg[:, at] = (acc * scale[:, 0:1]).astype(BF16)

    @pl.loop(0, width // tile_width)
    def _(c):
        at = aligned(c * tile_width, tile_width, tile_width)
        total = None
        for r in range(relations):
            part_r = jnp.dot(
                msg[r * rows : (r + 1) * rows, :], weights[r, :, at], preferred_element_type=F32
            )
            total = part_r if total is None else total + part_r
        pre[:, at] = total

    whole = pre[...]
    for k in range(groups):
        pre_send[k] = pack(whole, k * share, share).astype(BF16)

    piece_rows = rows // 4

    def reduce_pre(i, p):
        at = slice(p * piece_rows, (p + 1) * piece_rows)
        return pltpu.make_async_remote_copy(
            src_ref=pre_send.at[rel(i), at, :], dst_ref=pre_recv.at[i, at, :],
            send_sem=p_send.at[i, p], recv_sem=p_recv.at[i, p],
            device_id=(rel(i), me), device_id_type=MESH,
        )

    for p in range(2):
        for i in range(1, groups):
            reduce_pre(i, p).start()

    for r in range(relations):
        turned = msg[r * rows : (r + 1) * rows, :].astype(F32).T
        cut = turned.reshape(n, width // n, rows)
        for c in range(2):
            msg_t[r, c] = jnp.concatenate([cut[z * 2 + c] for z in range(chips)], axis=0).astype(BF16)

    for k in range(groups):
        @pl.when(grp == k)
        def _():
            cot_own[...] = pack(cot[...].astype(F32), k * share, share)
            piece = bias[:, k * share : (k + 1) * share]
            bias_own[...] = jnp.concatenate([piece, piece], axis=1)

    def gather_gp(i, p):
        at = slice(p * piece_rows, (p + 1) * piece_rows)
        return pltpu.make_async_remote_copy(
            src_ref=gp_all.at[grp, at, :], dst_ref=gp_all.at[grp, at, :],
            send_sem=g_send.at[i, p], recv_sem=g_recv.at[i, p],
            device_id=(rel(i), me), device_id_type=MESH,
        )

    for p in range(2):
        at = slice(p * piece_rows, (p + 1) * piece_rows)
        total = pre_send[grp, at, :].astype(F32)
        for i in range(1, groups):
            reduce_pre(i, p).wait_recv()
            total = total + pre_recv[i, at, :].astype(F32)
        pre_act = total + bias_own[...]
        sigmoid = jax.nn.sigmoid(pre_act)
        derivative = sigmoid * (1.0 + pre_act * (1.0 - sigmoid))
        gp_all[grp, at, :] = (cot_own[at, :] * derivative).astype(BF16)
        for i in range(1, groups):
            gather_gp(i, p).start()
        out[at, :] = (pre_act * sigmoid).astype(BF16)

    for p in range(2):
        for i in range(1, groups):
            gather_gp(i, p).wait_recv()
    half = rows // 2
    for h in range(2):
        gp[h * half : (h + 1) * half, :] = jnp.concatenate(
            [gp_all[k][:, h * share : (h + 1) * share].astype(F32) for k in range(groups)], axis=1
        ).astype(BF16)

    def weight_chunks(r, c):
        product = jnp.dot(msg_t[r, c], gp[...], preferred_element_type=F32)
        return product.reshape(chips, width // n, width)

    def pair(z):
        return pltpu.make_async_remote_copy(
            src_ref=wg_pair.at[z], dst_ref=wg_pair_recv.at[z],
            send_sem=w_send.at[z], recv_sem=w_recv.at[z],
            device_id=(grp, partner), device_id_type=MESH,
        )

    for r in range(relations):
        wg_pair[:, r] = weight_chunks(r, 1 - core).astype(BF16)

    @pl.loop(0, chips)
    def _(z):
        pair(z).start()

    for r in range(relations):
        wg_own[:, r] = weight_chunks(r, core)

    def climb(d):
        return pltpu.make_async_remote_copy(
            src_ref=up_send.at[d], dst_ref=up_recv.at[d],
            send_sem=u_send.at[d], recv_sem=u_recv.at[d],
            device_id=(grp, jnp.minimum(chip + 1, chips - 1) * 2 + core), device_id_type=MESH,
        )

    def descend(d):
        return pltpu.make_async_remote_copy(
            src_ref=down_send.at[d], dst_ref=down_recv.at[d],
            send_sem=v_send.at[d], recv_sem=v_recv.at[d],
            device_id=(grp, jnp.maximum(chip - 1, 0) * 2 + core), device_id_type=MESH,
        )

    def chip_sum(r, z):
        return wg_own[z, r] + wg_pair_recv[z, r].astype(F32)

    def line_step(step):
        @pl.when(step >= chip)
        def _():
            d = chips - 1 - step + chip

            @pl.when(chip > 0)
            def _():
                climb(d).wait_recv()
                for r in range(relations):
                    up_send[d, r] = (chip_sum(r, d) + up_recv[d, r].astype(F32)).astype(BF16)

            @pl.when(chip == 0)
            def _():
                for r in range(relations):
                    up_send[d, r] = chip_sum(r, d).astype(BF16)

            climb(d).start()

        @pl.when(step >= chips - 1 - chip)
        def _():
            d = step - chips + 1 + chip

            @pl.when(chip < chips - 1)
            def _():
                descend(d).wait_recv()
                for r in range(relations):
                    down_send[d, r] = (chip_sum(r, d) + down_recv[d, r].astype(F32)).astype(BF16)

            @pl.when(chip == chips - 1)
            def _():
                for r in range(relations):
                    down_send[d, r] = chip_sum(r, d).astype(BF16)

            descend(d).start()

    @pl.loop(0, chips)
    def _(z):
        pair(z).wait_recv()

    line_step(0)

    @pl.loop(0, width // tile_width)
    def _(c):
        at = aligned(c * tile_width, tile_width, tile_width)
        for r in range(relations):
            rows_r = slice(r * rows, (r + 1) * rows)
            grads = lax.dot_general(
                gp[...], weights[r, at, :],
                (((1,), (1,)), ((), ())), preferred_element_type=F32,
            )
            gm[rows_r, at] = (grads * scale[rows_r, 0:1]).astype(BF16)

    def reduce_part(o, i):
        return pltpu.make_async_remote_copy(
            src_ref=part.at[o, aligned(rel(i) * quarter, quarter, quarter), :],
            dst_ref=part_recv.at[i, o],
            send_sem=d_send.at[o, i], recv_sem=d_recv.at[o, i],
            device_id=(rel(i), me), device_id_type=MESH,
        )

    batch = 4

    @pl.loop(0, n // batch)
    def _(e):
        product = jnp.dot(
            adj_t[pl.ds(pl.multiple_of(e * batch * blk, blk), batch * blk), :], gm[...],
            preferred_element_type=F32,
        )
        part[pl.ds(e * batch, batch)] = product.reshape(batch, blk, width).astype(BF16)
        for v in range(batch):
            for i in range(1, groups):
                reduce_part(e * batch + v, i).start()

    @pl.loop(1, chips - 1)
    def _(step):
        line_step(step)

    for r in range(relations):
        grad_w[r] = chip_sum(r, chip)

    def give_back(j):
        return pltpu.make_async_remote_copy(
            src_ref=part_sum.at[tgt(j)], dst_ref=part_back.at[me],
            send_sem=e_send.at[j], recv_sem=e_recv.at[j],
            device_id=(grp, tgt(j)), device_id_type=MESH,
        )

    def reduced(o):
        total = part[o, aligned(grp * quarter, quarter, quarter), :].astype(F32)
        for i in range(1, groups):
            reduce_part(o, i).wait_recv()
            total = total + part_recv[i, o].astype(F32)
        return total.astype(BF16)

    part_back[me] = reduced(me)

    @pl.loop(1, n)
    def _(j):
        part_sum[tgt(j)] = reduced(tgt(j))
        give_back(j).start()

    @pl.when(chip > 0)
    def _():
        climb(chip).wait_recv()
        for r in range(relations):
            grad_w[r] = grad_w[r] + up_recv[chip, r].astype(F32)

    @pl.when(chip < chips - 1)
    def _():
        descend(chip).wait_recv()
        for r in range(relations):
            grad_w[r] = grad_w[r] + down_recv[chip, r].astype(F32)

    @pl.loop(1, n)
    def _(j):
        give_back(j).wait_recv()

    for k in range(sections):
        grad_f[k] = jnp.zeros((quarter, width), F32)

    @pl.loop(0, n)
    def _(t):
        wanted = table[t, me]
        addend = part_back[t].astype(F32)
        for k in range(sections):
            grad_f[k] = grad_f[k] + addend * is_one(wanted == k)

    fetch_pair.wait_send()

    @pl.loop(2, n)
    def _(j):
        fetch(j).wait_send()
        for way in range(4):
            spread(j, way).wait_send()

    @pl.loop(1, n)
    def _(j):
        give_back(j).wait_send()

    for i in range(1, groups):
        for p in range(2):
            reduce_pre(i, p).wait_send()
            gather_gp(i, p).wait_send()

    @pl.loop(0, n)
    def _(o):
        for i in range(1, groups):
            reduce_part(o, i).wait_send()

    @pl.loop(0, chips)
    def _(z):
        pair(z).wait_send()

        @pl.when(z > chip)
        def _():
            climb(z).wait_send()

        @pl.when(z < chip)
        def _():
            descend(z).wait_send()


def per_device(
    n, groups,
    features, weights, bias, cotangent, tile_values, tile_count, tile_slot, source_blocks,
):
    rows, width = features.shape
    relations, _, slot_total, blk = tile_values.shape
    sections = rows // blk
    quarter, share, chunk, chips = blk // groups, width // groups, width // n, n // 2
    half = rows // 2
    vmem = pl.BlockSpec(memory_space=pltpu.VMEM)
    smem = pl.BlockSpec(memory_space=pltpu.SMEM)
    anywhere = pl.BlockSpec(memory_space=pl.ANY)
    dma = pltpu.SemaphoreType.DMA
    out, grad_w, grad_f = pl.pallas_call(
        functools.partial(kernel, n, groups),
        out_shape=(
            jax.ShapeDtypeStruct((half, 2 * share), BF16),
            jax.ShapeDtypeStruct((relations, chunk, width), F32),
            jax.ShapeDtypeStruct((sections, quarter, width), F32),
        ),
        in_specs=[smem, smem, smem, vmem, vmem, vmem, anywhere, anywhere],
        out_specs=(vmem, vmem, vmem),
        scratch_shapes=[
            pltpu.VMEM((relations, width, width), BF16),
            pltpu.VMEM((relations, rows * slot_total, blk), jnp.int32),
            pltpu.VMEM((n, quarter, width), BF16),
            pltpu.VMEM((blk, width), BF16),
            pltpu.VMEM((slot_total, blk, blk), jnp.int32),
            pltpu.VMEM((n * blk, width), BF16),
            pltpu.VMEM((relations * rows, n * blk), BF16),
            pltpu.VMEM((relations * rows, 128), F32),
            pltpu.VMEM((relations * rows, width), BF16),
            pltpu.VMEM((relations, 2, chips * chunk, rows), BF16),
            pltpu.VMEM((chips, relations, chunk, width), F32),
            pltpu.VMEM((n * blk, relations * rows), BF16),
            pltpu.VMEM((rows, width), F32),
            pltpu.VMEM((groups, half, 2 * share), BF16),
            pltpu.VMEM((groups, half, 2 * share), BF16),
            pltpu.VMEM((half, 2 * share), F32),
            pltpu.VMEM((1, 2 * share), F32),
            pltpu.VMEM((groups, half, 2 * share), BF16),
            pltpu.VMEM((rows, width), BF16),
            pltpu.VMEM((relations * rows, width), BF16),
            pltpu.VMEM((n, blk, width), BF16),
            pltpu.VMEM((groups, n, quarter, width), BF16),
            pltpu.VMEM((n, quarter, width), BF16),
            pltpu.VMEM((n, quarter, width), BF16),
            pltpu.VMEM((chips, relations, chunk, width), BF16),
            pltpu.VMEM((chips, relations, chunk, width), BF16),
            pltpu.VMEM((chips, relations, chunk, width), BF16),
            pltpu.VMEM((chips, relations, chunk, width), BF16),
            pltpu.VMEM((chips, relations, chunk, width), BF16),
            pltpu.VMEM((chips, relations, chunk, width), BF16),
            dma((2,)),
            dma((n,)), dma((n,)),
            dma((n, 4)), dma((n, 4)),
            dma((groups, 2)), dma((groups, 2)),
            dma((groups, 2)), dma((groups, 2)),
            dma((n, groups)), dma((n, groups)),
            dma((n,)), dma((n,)),
            dma((chips,)), dma((chips,)),
            dma((chips,)), dma((chips,)),
            dma((chips,)), dma((chips,)),
        ],
        compiler_params=pltpu.CompilerParams(
            collective_id=0, has_side_effects=True, vmem_limit_bytes=60 << 20
        ),
        name="layer",
    )(
        source_blocks, tile_count, tile_slot,
        features, cotangent, bias.reshape(1, width),
        tile_values.reshape(relations, rows * slot_total, blk), weights,
    )
    output = out.reshape(half, 2, share).swapaxes(0, 1).reshape(rows, share)
    return (output, grad_w, grad_f)


def solution(mesh):
    placed = (
        P("tgt", None),
        P("rel", None, None),
        P(),
        P("tgt", None),
        P("rel", "tgt", None, None),
        P("rel", "tgt"),
        P("rel", "tgt", None),
        P(),
    )
    return jax.shard_map(
        functools.partial(per_device, mesh.shape["tgt"], mesh.shape["rel"]),
        mesh=mesh,
        in_specs=placed,
        out_specs=(P("tgt", "rel"), P("rel", "tgt", None), P("tgt", "rel", None)),
        check_vma=False,
    )
```

```python
import functools

import jax
import jax.numpy as jnp
from jax import lax
from jax.experimental import pallas as pl
from jax.experimental.pallas import tpu as pltpu
from jax.sharding import PartitionSpec as P

MESH = pl.DeviceIdType.MESH
F32 = jnp.float32
BF16 = jnp.bfloat16


def aligned(start, size, multiple):
    return pl.ds(pl.multiple_of(start, multiple), size)


def is_one(condition):
    return condition.astype(jnp.int32).astype(F32)


def pack(value, first, width):
    half = value.shape[0] // 2
    return jnp.concatenate(
        [value[:half, first : first + width], value[half:, first : first + width]], axis=1
    )


def kernel(
    n, groups,
    table, counts, slots,
    feat, cot, bias, values_hbm, weights_hbm,
    out, grad_w, grad_f,
    weights, values, staged, partner_staged, masked, fetched, adj, scale, msg, msg_t, wg_own, adj_t, pre,
    pre_send, pre_recv, cot_own, active, bias_own, gp_all, gp, gm,
    part, part_recv, part_sum, part_back,
    wg_pair, wg_pair_recv, up_send, up_recv, down_send, down_recv,
    load_sem, a_send, a_recv, b_send, b_recv, p_send, p_recv, g_send, g_recv,
    d_send, d_recv, e_send, e_recv, w_send, w_recv, u_send, u_recv, v_send, v_recv,
):
    me = lax.axis_index("tgt")
    grp = lax.axis_index("rel")
    rows, width = feat.shape
    relations = weights.shape[0]
    slot_total = slots.shape[2]
    blk = values.shape[1] // (rows * slot_total) * values.shape[2]
    sections = rows // blk
    quarter = blk // groups
    share = width // groups
    chips = n // 2
    chip, core = me // 2, lax.rem(me, 2)

    def tgt(j):
        return lax.rem(chip + j // 2, chips) * 2 + lax.rem(core + lax.rem(j, 2), 2)

    def tgt_back(j):
        return lax.rem(chip + chips - j // 2, chips) * 2 + lax.rem(core + lax.rem(j, 2), 2)

    partner = chip * 2 + 1 - core
    row, column = grp // 2, lax.rem(grp, 2)
    beside = row * 2 + 1 - column
    above = (1 - row) * 2 + column

    def rel(i):
        return lax.rem(grp + i, groups)

    load_w = pltpu.make_async_copy(weights_hbm, weights, load_sem.at[0])
    load_v = pltpu.make_async_copy(values_hbm, values, load_sem.at[1])
    load_v.start()
    load_w.start()

    barrier = pltpu.get_barrier_semaphore()

    @pl.loop(1, n)
    def _(j):
        pl.semaphore_signal(barrier, inc=1, device_id=(grp, tgt(j)), device_id_type=MESH)

    for i in range(1, groups):
        pl.semaphore_signal(barrier, inc=1, device_id=(rel(i), me), device_id_type=MESH)

    @pl.loop(0, n)
    def _(t):
        total = jnp.zeros((quarter, width), F32)
        for k in range(sections):
            block = feat[aligned(k * blk + grp * quarter, quarter, quarter), :].astype(F32)
            total = total + block * is_one(table[t, me] == k)
        staged[t] = total.astype(BF16)

    def whole_block(t):
        total = jnp.zeros((blk, width), F32)
        for k in range(sections):
            total = total + feat[k * blk : (k + 1) * blk, :].astype(F32) * is_one(table[t, me] == k)
        return total.astype(BF16)

    fetched[aligned(me * blk, blk, blk), :] = whole_block(me)
    partner_staged[...] = whole_block(partner)
    pl.semaphore_wait(barrier, n - 1 + groups - 1)

    def fetch(j):
        return pltpu.make_async_remote_copy(
            src_ref=staged.at[tgt(j)],
            dst_ref=fetched.at[aligned(me * blk + grp * quarter, quarter, quarter), :],
            send_sem=a_send.at[j], recv_sem=a_recv.at[j],
            device_id=(grp, tgt(j)), device_id_type=MESH,
        )

    fetch_pair = pltpu.make_async_remote_copy(
        src_ref=partner_staged, dst_ref=fetched.at[aligned(me * blk, blk, blk), :],
        send_sem=a_send.at[1], recv_sem=a_recv.at[1],
        device_id=(grp, partner), device_id_type=MESH,
    )

    @pl.loop(2, n)
    def _(j):
        fetch(j).start()

    fetch_pair.start()

    def spread(j, way):
        size = quarter if way < 2 else quarter // 2
        source = (grp, grp, beside, above)[way]
        extra = quarter // 2 if way == 3 else 0
        peer = (beside, above, above, beside)[way]
        rows_at = aligned(tgt_back(j) * blk + source * quarter + extra, size, size)
        return pltpu.make_async_remote_copy(
            src_ref=fetched.at[rows_at, :], dst_ref=fetched.at[rows_at, :],
            send_sem=b_send.at[j, way], recv_sem=b_recv.at[j, way],
            device_id=(peer, me), device_id_type=MESH,
        )

    def pass_on(j):
        spread(j, 0).wait_recv()
        spread(j, 2).start()
        spread(j, 1).wait_recv()
        spread(j, 3).start()

    def arrive(j):
        fetch(j).wait_recv()
        spread(j, 0).start()
        spread(j, 1).start()

    load_v.wait()

    @pl.loop(0, relations * sections)
    def _(b):
        r, q = b // sections, lax.rem(b, sections)
        count = counts[r, q]

        def tile(s):
            start = (q * blk * slot_total) + s
            live = (s < count).astype(jnp.int32)
            return values[r, pl.ds(start, blk, stride=slot_total), :] * live

        total = jnp.zeros((blk, blk), jnp.int32)
        for s in range(slot_total):
            live_tile = tile(s)
            masked[s] = live_tile
            total = total + live_tile
        degree = jnp.sum(total.astype(F32), axis=1, keepdims=True)
        root = 1.0 / jnp.sqrt(jnp.maximum(degree, 1.0))
        scale[aligned(b * blk, blk, blk), :] = jnp.broadcast_to(root, (blk, 128))

        @pl.loop(0, n)
        def _(o):
            entry = jnp.zeros((blk, blk), jnp.int32)
            for s in range(slot_total):
                entry = entry + masked[s] * (slots[r, q, s] == o).astype(jnp.int32)
            wide = entry.astype(F32)
            adj[aligned(b * blk, blk, blk), aligned(o * blk, blk, blk)] = wide.astype(BF16)
            adj_t[aligned(o * blk, blk, blk), aligned(b * blk, blk, blk)] = wide.T.astype(BF16)

        arrive(b + 2)

    @pl.loop(relations * sections + 2, n)
    def _(j):
        arrive(j)
        pass_on(j - relations * sections)

    @pl.loop(n - relations * sections, n)
    def _(j):
        pass_on(j)

    load_w.wait()
    fetch_pair.wait_recv()

    @pl.loop(2, n)
    def _(j):
        spread(j, 2).wait_recv()
        spread(j, 3).wait_recv()

    tile_width = 256

    @pl.loop(0, width // tile_width)
    def _(c):
        at = aligned(c * tile_width, tile_width, tile_width)
        acc = jnp.dot(adj[...], fetched[:, at], preferred_element_type=F32)
        msg[:, at] = (acc * scale[:, 0:1]).astype(BF16)

    @pl.loop(0, width // tile_width)
    def _(c):
        at = aligned(c * tile_width, tile_width, tile_width)
        total = None
        for r in range(relations):
            part_r = jnp.dot(
                msg[r * rows : (r + 1) * rows, :], weights[r, :, at], preferred_element_type=F32
            )
            total = part_r if total is None else total + part_r
        pre[:, at] = total

    whole = pre[...]
    for k in range(groups):
        pre_send[k] = pack(whole, k * share, share).astype(BF16)

    piece_rows = rows // 4

    def reduce_pre(i, p):
        at = slice(p * piece_rows, (p + 1) * piece_rows)
        return pltpu.make_async_remote_copy(
            src_ref=pre_send.at[rel(i), at, :], dst_ref=pre_recv.at[i, at, :],
            send_sem=p_send.at[i, p], recv_sem=p_recv.at[i, p],
            device_id=(rel(i), me), device_id_type=MESH,
        )

    for p in range(2):
        for i in range(1, groups):
            reduce_pre(i, p).start()

    for r in range(relations):
        turned = msg[r * rows : (r + 1) * rows, :].astype(F32).T
        cut = turned.reshape(n, width // n, rows)
        for c in range(2):
            msg_t[r, c] = jnp.concatenate([cut[z * 2 + c] for z in range(chips)], axis=0).astype(BF16)

    for k in range(groups):
        @pl.when(grp == k)
        def _():
            cot_own[...] = pack(cot[...].astype(F32), k * share, share)
            piece = bias[...].reshape(1, width)[:, k * share : (k + 1) * share]
            bias_own[...] = jnp.concatenate([piece, piece], axis=1)

    def gather_gp(i, p):
        at = slice(p * piece_rows, (p + 1) * piece_rows)
        return pltpu.make_async_remote_copy(
            src_ref=gp_all.at[grp, at, :], dst_ref=gp_all.at[grp, at, :],
            send_sem=g_send.at[i, p], recv_sem=g_recv.at[i, p],
            device_id=(rel(i), me), device_id_type=MESH,
        )

    for p in range(2):
        at = slice(p * piece_rows, (p + 1) * piece_rows)
        total = pre_send[grp, at, :].astype(F32)
        for i in range(1, groups):
            reduce_pre(i, p).wait_recv()
            total = total + pre_recv[i, at, :].astype(F32)
        pre_act = total + bias_own[...]
        sigmoid = jax.nn.sigmoid(pre_act)
        derivative = sigmoid * (1.0 + pre_act * (1.0 - sigmoid))
        gp_all[grp, at, :] = (cot_own[at, :] * derivative).astype(BF16)
        for i in range(1, groups):
            gather_gp(i, p).start()
        active[at, :] = pre_act * sigmoid

    upright = active[...].T
    for h in range(2):
        out[:, h * (rows // 2) : (h + 1) * (rows // 2)] = upright[h * share : (h + 1) * share].astype(BF16)

    for p in range(2):
        for i in range(1, groups):
            gather_gp(i, p).wait_recv()
    half = rows // 2
    for h in range(2):
        gp[h * half : (h + 1) * half, :] = jnp.concatenate(
            [gp_all[k][:, h * share : (h + 1) * share].astype(F32) for k in range(groups)], axis=1
        ).astype(BF16)

    def weight_chunks(r, c):
        product = jnp.dot(msg_t[r, c], gp[...], preferred_element_type=F32)
        return product.reshape(chips, width // n, width)

    def pair(z):
        return pltpu.make_async_remote_copy(
            src_ref=wg_pair.at[z], dst_ref=wg_pair_recv.at[z],
            send_sem=w_send.at[z], recv_sem=w_recv.at[z],
            device_id=(grp, partner), device_id_type=MESH,
        )

    for r in range(relations):
        wg_pair[:, r] = weight_chunks(r, 1 - core).astype(BF16)

    @pl.loop(0, chips)
    def _(z):
        pair(z).start()

    for r in range(relations):
        wg_own[:, r] = weight_chunks(r, core)

    def climb(d):
        return pltpu.make_async_remote_copy(
            src_ref=up_send.at[d], dst_ref=up_recv.at[d],
            send_sem=u_send.at[d], recv_sem=u_recv.at[d],
            device_id=(grp, jnp.minimum(chip + 1, chips - 1) * 2 + core), device_id_type=MESH,
        )

    def descend(d):
        return pltpu.make_async_remote_copy(
            src_ref=down_send.at[d], dst_ref=down_recv.at[d],
            send_sem=v_send.at[d], recv_sem=v_recv.at[d],
            device_id=(grp, jnp.maximum(chip - 1, 0) * 2 + core), device_id_type=MESH,
        )

    def chip_sum(r, z):
        return wg_own[z, r] + wg_pair_recv[z, r].astype(F32)

    def line_step(step):
        @pl.when(step >= chip)
        def _():
            d = chips - 1 - step + chip

            @pl.when(chip > 0)
            def _():
                climb(d).wait_recv()
                for r in range(relations):
                    up_send[d, r] = (chip_sum(r, d) + up_recv[d, r].astype(F32)).astype(BF16)

            @pl.when(chip == 0)
            def _():
                for r in range(relations):
                    up_send[d, r] = chip_sum(r, d).astype(BF16)

            climb(d).start()

        @pl.when(step >= chips - 1 - chip)
        def _():
            d = step - chips + 1 + chip

            @pl.when(chip < chips - 1)
            def _():
                descend(d).wait_recv()
                for r in range(relations):
                    down_send[d, r] = (chip_sum(r, d) + down_recv[d, r].astype(F32)).astype(BF16)

            @pl.when(chip == chips - 1)
            def _():
                for r in range(relations):
                    down_send[d, r] = chip_sum(r, d).astype(BF16)

            descend(d).start()

    @pl.loop(0, chips)
    def _(z):
        pair(z).wait_recv()

    line_step(0)

    @pl.loop(0, width // tile_width)
    def _(c):
        at = aligned(c * tile_width, tile_width, tile_width)
        for r in range(relations):
            rows_r = slice(r * rows, (r + 1) * rows)
            grads = lax.dot_general(
                gp[...], weights[r, at, :],
                (((1,), (1,)), ((), ())), preferred_element_type=F32,
            )
            gm[rows_r, at] = (grads * scale[rows_r, 0:1]).astype(BF16)

    def reduce_part(o, i):
        return pltpu.make_async_remote_copy(
            src_ref=part.at[o, aligned(rel(i) * quarter, quarter, quarter), :],
            dst_ref=part_recv.at[i, o],
            send_sem=d_send.at[o, i], recv_sem=d_recv.at[o, i],
            device_id=(rel(i), me), device_id_type=MESH,
        )

    @pl.loop(1, chips + 1)
    def _(e):
        z = lax.rem(chip + e, chips)
        product = jnp.dot(
            adj_t[aligned(z * 2 * blk, 2 * blk, blk), :], gm[...], preferred_element_type=F32
        )
        for v in range(2):
            o = z * 2 + v
            part[o] = product[v * blk : (v + 1) * blk].astype(BF16)
            for i in range(1, groups):
                reduce_part(o, i).start()

    def give_back(j):
        return pltpu.make_async_remote_copy(
            src_ref=part_sum.at[tgt(j)], dst_ref=part_back.at[me],
            send_sem=e_send.at[j], recv_sem=e_recv.at[j],
            device_id=(grp, tgt(j)), device_id_type=MESH,
        )

    def reduced(o):
        total = part[o, aligned(grp * quarter, quarter, quarter), :].astype(F32)
        for i in range(1, groups):
            reduce_part(o, i).wait_recv()
            total = total + part_recv[i, o].astype(F32)
        return total.astype(BF16)

    def send_reduced(j):
        part_sum[tgt(j)] = reduced(tgt(j))
        give_back(j).start()

    @pl.loop(1, chips - 1)
    def _(step):
        line_step(step)
        send_reduced(2 * step)
        send_reduced(2 * step + 1)

    for r in range(relations):
        grad_w[r] = chip_sum(r, chip)

    send_reduced(n - 2)
    send_reduced(n - 1)
    send_reduced(1)
    part_back[me] = reduced(me)

    @pl.when(chip > 0)
    def _():
        climb(chip).wait_recv()
        for r in range(relations):
            grad_w[r] = grad_w[r] + up_recv[chip, r].astype(F32)

    @pl.when(chip < chips - 1)
    def _():
        descend(chip).wait_recv()
        for r in range(relations):
            grad_w[r] = grad_w[r] + down_recv[chip, r].astype(F32)

    @pl.loop(1, n)
    def _(j):
        give_back(j).wait_recv()

    for k in range(sections):
        grad_f[k] = jnp.zeros((quarter, width), F32)

    @pl.loop(0, n)
    def _(t):
        wanted = table[t, me]
        addend = part_back[t].astype(F32)
        for k in range(sections):
            grad_f[k] = grad_f[k] + addend * is_one(wanted == k)

    fetch_pair.wait_send()

    @pl.loop(2, n)
    def _(j):
        fetch(j).wait_send()
        for way in range(4):
            spread(j, way).wait_send()

    @pl.loop(1, n)
    def _(j):
        give_back(j).wait_send()

    for i in range(1, groups):
        for p in range(2):
            reduce_pre(i, p).wait_send()
            gather_gp(i, p).wait_send()

    @pl.loop(0, n)
    def _(o):
        for i in range(1, groups):
            reduce_part(o, i).wait_send()

    @pl.loop(0, chips)
    def _(z):
        pair(z).wait_send()

        @pl.when(z > chip)
        def _():
            climb(z).wait_send()

        @pl.when(z < chip)
        def _():
            descend(z).wait_send()


def hand_over(out_in, grad_w_in, grad_f_in, out, grad_w, grad_f):
    out[...] = out_in[...]
    grad_w[...] = grad_w_in[...]
    grad_f[...] = grad_f_in[...]


def per_device(
    n, groups,
    features, weights, bias, cotangent, tile_values, tile_count, tile_slot, source_blocks,
):
    rows, width = features.shape
    relations, _, slot_total, blk = tile_values.shape
    sections = rows // blk
    quarter, share, chunk, chips = blk // groups, width // groups, width // n, n // 2
    half = rows // 2
    vmem = pl.BlockSpec(memory_space=pltpu.VMEM)
    smem = pl.BlockSpec(memory_space=pltpu.SMEM)
    anywhere = pl.BlockSpec(memory_space=pl.ANY)
    dma = pltpu.SemaphoreType.DMA
    out, grad_w, grad_f = pl.pallas_call(
        functools.partial(kernel, n, groups),
        out_shape=(
            jax.ShapeDtypeStruct((share, rows), BF16),
            jax.ShapeDtypeStruct((relations, chunk, width), F32),
            jax.ShapeDtypeStruct((sections, quarter, width), F32),
        ),
        in_specs=[smem, smem, smem, vmem, vmem, vmem, anywhere, anywhere],
        out_specs=(vmem, vmem, vmem),
        scratch_shapes=[
            pltpu.VMEM((relations, width, width), BF16),
            pltpu.VMEM((relations, rows * slot_total, blk), jnp.int32),
            pltpu.VMEM((n, quarter, width), BF16),
            pltpu.VMEM((blk, width), BF16),
            pltpu.VMEM((slot_total, blk, blk), jnp.int32),
            pltpu.VMEM((n * blk, width), BF16),
            pltpu.VMEM((relations * rows, n * blk), BF16),
            pltpu.VMEM((relations * rows, 128), F32),
            pltpu.VMEM((relations * rows, width), BF16),
            pltpu.VMEM((relations, 2, chips * chunk, rows), BF16),
            pltpu.VMEM((chips, relations, chunk, width), F32),
            pltpu.VMEM((n * blk, relations * rows), BF16),
            pltpu.VMEM((rows, width), F32),
            pltpu.VMEM((groups, half, 2 * share), BF16),
            pltpu.VMEM((groups, half, 2 * share), BF16),
            pltpu.VMEM((half, 2 * share), F32),
            pltpu.VMEM((half, 2 * share), F32),
            pltpu.VMEM((1, 2 * share), F32),
            pltpu.VMEM((groups, half, 2 * share), BF16),
            pltpu.VMEM((rows, width), BF16),
            pltpu.VMEM((relations * rows, width), BF16),
            pltpu.VMEM((n, blk, width), BF16),
            pltpu.VMEM((groups, n, quarter, width), BF16),
            pltpu.VMEM((n, quarter, width), BF16),
            pltpu.VMEM((n, quarter, width), BF16),
            pltpu.VMEM((chips, relations, chunk, width), BF16),
            pltpu.VMEM((chips, relations, chunk, width), BF16),
            pltpu.VMEM((chips, relations, chunk, width), BF16),
            pltpu.VMEM((chips, relations, chunk, width), BF16),
            pltpu.VMEM((chips, relations, chunk, width), BF16),
            pltpu.VMEM((chips, relations, chunk, width), BF16),
            dma((2,)),
            dma((n,)), dma((n,)),
            dma((n, 4)), dma((n, 4)),
            dma((groups, 2)), dma((groups, 2)),
            dma((groups, 2)), dma((groups, 2)),
            dma((n, groups)), dma((n, groups)),
            dma((n,)), dma((n,)),
            dma((chips,)), dma((chips,)),
            dma((chips,)), dma((chips,)),
            dma((chips,)), dma((chips,)),
        ],
        compiler_params=pltpu.CompilerParams(
            collective_id=0, has_side_effects=True, vmem_limit_bytes=60 << 20
        ),
        name="layer",
    )(
        source_blocks, tile_count, tile_slot,
        features, cotangent, bias,
        tile_values.reshape(relations, rows * slot_total, blk), weights,
    )
    results = (out, grad_w, grad_f)
    out, grad_w, grad_f = pl.pallas_call(
        hand_over,
        out_shape=tuple(jax.ShapeDtypeStruct(x.shape, x.dtype) for x in results),
        in_specs=[vmem] * 3,
        out_specs=(vmem,) * 3,
        name="hand_over",
    )(*results)
    return (out.T, grad_w, grad_f)


def solution(mesh):
    placed = (
        P("tgt", None),
        P("rel", None, None),
        P(),
        P("tgt", None),
        P("rel", "tgt", None, None),
        P("rel", "tgt"),
        P("rel", "tgt", None),
        P(),
    )
    return jax.shard_map(
        functools.partial(per_device, mesh.shape["tgt"], mesh.shape["rel"]),
        mesh=mesh,
        in_specs=placed,
        out_specs=(P("tgt", "rel"), P("rel", "tgt", None), P("tgt", "rel", None)),
        check_vma=False,
    )
```
